16 devices in a mesh: tp: 2 (over z), dp: 8 (over y, x, core).
Axes of the slice: x: 2, y: 2, z: 2, core: 2. Of those that a mesh axis runs over, the one named last changes fastest.
Arguments:
- hidden: bfloat16 [8192, 2048], P('dp')
- norm_w: bfloat16 [2048], replicated
- emb_table: bfloat16 [49152, 2048], P('tp')
- teacher: bfloat16 [8192, 49152], P('dp', 'tp')
- loss_mask: int32 [8192], P('dp')
Outputs:
- output 1: float32 [], replicated
- output 2: bfloat16 [8192, 2048], P('dp')
- output 3: float32 [49152, 2048], P('tp', 'dp')
- output 4: float32 [2048], replicated
All inputs are finite; a program needn't handle non-finite values.
Results may differ from the reference program's by a relative error of at most 0.00103826.
Values sent between devices are 32-bit elements.
A program may use at most 1 GiB of HBM per device.

```python
import jax
import jax.numpy as jnp
from jax import lax

MODEL_DIM = 2048
VOCAB_SIZE = 49152
TOK_DEV = 1024
DP_SHARDS = 8
TOKENS = TOK_DEV * DP_SHARDS
SOFT_CAP = 30.0
NORM_EPS = 1e-6


def setup_inputs(seed: int = 0) -> dict:
    base_key = jax.random.key(seed)
    key_list = jax.random.split(base_key, 6)
    hidden = jax.random.normal(key_list[0], (TOKENS, MODEL_DIM), jnp.float32)
    norm_w = 0.5 * jax.random.normal(key_list[1], (MODEL_DIM,), jnp.float32)
    mean_dir = jax.random.normal(key_list[2], (MODEL_DIM,), jnp.float32)
    emb_noise = jax.random.normal(key_list[3], (VOCAB_SIZE, MODEL_DIM), jnp.float32)
    emb_table = (18.0 * mean_dir[None, :] + 1.5 * emb_noise) * (MODEL_DIM ** -0.5)
    teacher = 2.0 * jax.random.normal(key_list[4], (TOKENS, VOCAB_SIZE), jnp.float32)
    lengths = jax.random.randint(key_list[5], (DP_SHARDS,), 1, TOK_DEV + 1)
    lengths = jnp.where(jnp.arange(DP_SHARDS) == 0, TOK_DEV, lengths)
    loss_mask = (jnp.arange(TOK_DEV)[None, :] < lengths[:, None]).astype(jnp.int32)
    return {'hidden': hidden.astype(jnp.bfloat16), 'norm_w': norm_w.astype(jnp.bfloat16), 'emb_table': emb_table.astype(jnp.bfloat16), 'teacher': teacher.astype(jnp.bfloat16), 'loss_mask': loss_mask.reshape(TOKENS)}


def rms_norm(hid_f32, scale_f32):
    inv_rms = lax.rsqrt(jnp.mean(hid_f32 * hid_f32, axis=-1, keepdims=True) + NORM_EPS)
    return hid_f32 * inv_rms * (1.0 + scale_f32)


def reference(hidden, norm_w, emb_table, teacher, loss_mask):
    mask_f32 = loss_mask.astype(jnp.float32)
    weights = mask_f32 / jnp.sum(mask_f32)
    scale_f32 = norm_w.astype(jnp.float32)

    def block_step(acc_state, blk_inputs):
        emb_acc, scale_acc = acc_state
        hid_blk, teach_blk, weight_blk = blk_inputs
        normed_f32, norm_pull = jax.vjp(rms_norm, hid_blk.astype(jnp.float32), scale_f32)
        normed = normed_f32.astype(jnp.bfloat16)
        raw_logit = jnp.dot(normed, emb_table.T, preferred_element_type=jnp.float32)
        tanh_val = jnp.tanh(raw_logit / SOFT_CAP)
        capped = SOFT_CAP * tanh_val
        log_stu = jax.nn.log_softmax(capped, axis=-1)
        log_tea = jax.nn.log_softmax(teach_blk.astype(jnp.float32), axis=-1)
        prob_tea = jnp.exp(log_tea)
        kl_tok = jnp.sum(prob_tea * (log_tea - log_stu), axis=-1)
        loss_part = jnp.sum(weight_blk * kl_tok)
        d_raw = ((jnp.exp(log_stu) - prob_tea) * weight_blk[:, None] * (1.0 - tanh_val * tanh_val)).astype(jnp.bfloat16)
        grad_normed = jnp.dot(d_raw, emb_table, preferred_element_type=jnp.float32)
        emb_acc = emb_acc + jnp.dot(d_raw.T, normed, preferred_element_type=jnp.float32)
        grad_hid, grad_scale = norm_pull(grad_normed)
        return (emb_acc, scale_acc + grad_scale), (loss_part, grad_hid.astype(jnp.bfloat16))

    blocks_in = (hidden.reshape(DP_SHARDS, TOK_DEV, MODEL_DIM), teacher.reshape(DP_SHARDS, TOK_DEV, VOCAB_SIZE), weights.reshape(DP_SHARDS, TOK_DEV))
    start_acc = (jnp.zeros((VOCAB_SIZE, MODEL_DIM), jnp.float32), jnp.zeros((MODEL_DIM,), jnp.float32))
    final_acc, per_block = lax.scan(block_step, start_acc, blocks_in)
    d_emb, d_norm_w = final_acc
    loss_parts, grad_hid = per_block
    return jnp.sum(loss_parts), grad_hid.reshape(TOKENS, MODEL_DIM), d_emb, d_norm_w
```

```python
import functools

import jax
import jax.numpy as jnp
from jax import lax
from jax.experimental import pallas as pl
from jax.experimental.pallas import tpu as pltpu
from jax.sharding import PartitionSpec as P

SOFT_CAP = 30.0
NORM_EPS = 1e-6
LANES = 128
SUB = 256
FWD_SUB = 512
NSLOT = 8
MESH = pl.DeviceIdType.MESH
NT = (((1,), (1,)), ((), ()))


def rms_norm(hid_f32, scale_f32):
    inv_rms = lax.rsqrt(jnp.mean(hid_f32 * hid_f32, axis=-1, keepdims=True) + NORM_EPS)
    return hid_f32 * inv_rms * (1.0 + scale_f32)


def stats_kernel(steps, g_ref, e_ref, ta_ref, tb_ref, out_ref, ra, rb, mx, st, su, ss):
    i = pl.program_id(0)
    sub = ra.shape[1]

    @pl.when(i == 0)
    def _():
        mx[...] = jnp.full_like(mx, -jnp.inf)
        for ref in (st, su, ss):
            ref[...] = jnp.zeros_like(ref)

    def stats(pairs, rows):
        parts = [(r, t, slice(c * LANES, (c + 1) * LANES)) for r, t in pairs for c in range(sub // LANES)]
        old = mx[rows]
        new = old
        for _, t_ref, cols in parts:
            new = jnp.maximum(new, t_ref[rows, cols].astype(jnp.float32))
        keep = jnp.exp(old - new)
        mx[rows] = new
        t_sum = st[rows] * keep
        u_sum = su[rows] * keep
        s_sum = ss[rows]
        for r_ref, t_ref, cols in parts:
            z = SOFT_CAP * jnp.tanh(r_ref[rows, cols] * (1.0 / SOFT_CAP))
            s_sum += jnp.exp(z)
            t = t_ref[rows, cols].astype(jnp.float32)
            te = jnp.exp(t - new)
            t_sum += te
            u_sum += te * (t - z)
        st[rows] = t_sum
        su[rows] = u_sum
        ss[rows] = s_sum

    n_chunk = 4
    m = g_ref.shape[0] // n_chunk
    for q in range(n_chunk):
        rows = slice(q * m, (q + 1) * m)
        r = lax.dot_general(g_ref[rows], e_ref[...], NT, preferred_element_type=jnp.float32)
        ra[rows] = r[:, 0:sub]
        rb[rows] = r[:, sub:]
        stats([(ra, ta_ref), (rb, tb_ref)], rows)

    @pl.when(i == steps - 1)
    def _():
        top = jnp.max(mx[...], axis=1, keepdims=True)
        keep = jnp.exp(mx[...] - top)
        out_ref[0] = jnp.broadcast_to(top, mx.shape)
        out_ref[1] = jnp.broadcast_to(jnp.sum(st[...] * keep, axis=1, keepdims=True), mx.shape)
        out_ref[2] = jnp.broadcast_to(jnp.sum(su[...] * keep, axis=1, keepdims=True), mx.shape)
        out_ref[3] = jnp.broadcast_to(jnp.sum(ss[...], axis=1, keepdims=True), mx.shape)


def forward_stats(g, emb, teach):
    rows, width = g.shape
    vocab = emb.shape[0]
    steps = vocab // (2 * FWD_SUB)
    return pl.pallas_call(
        functools.partial(stats_kernel, steps),
        grid=(steps,),
        out_shape=jax.ShapeDtypeStruct((4, rows, LANES), jnp.float32),
        in_specs=[
            pl.BlockSpec((rows, width), lambda i: (0, 0), pipeline_mode=pl.Buffered(1)),
            pl.BlockSpec((2 * FWD_SUB, width), lambda i: (i, 0)),
            pl.BlockSpec((rows, FWD_SUB), lambda i: (0, 2 * i)),
            pl.BlockSpec((rows, FWD_SUB), lambda i: (0, 2 * i + 1)),
        ],
        out_specs=pl.BlockSpec((4, rows, LANES), lambda i: (0, 0, 0)),
        scratch_shapes=[pltpu.VMEM((rows, FWD_SUB), jnp.float32)] * 2 + [pltpu.VMEM((rows, LANES), jnp.float32)] * 4,
        compiler_params=pltpu.CompilerParams(
            dimension_semantics=("arbitrary",), vmem_limit_bytes=60 * 1024 * 1024
        ),
        cost_estimate=pl.CostEstimate(
            flops=2 * rows * width * vocab, bytes_accessed=2 * vocab * (width + rows), transcendentals=3 * rows * vocab
        ),
        name="fwd_stats",
    )(g, emb, teach, teach)


def grad_kernel(blocks, base, g_ref, x_ref, w_ref, row_ref, mine_ref, e_ref, t_ref, ex_ref, tx_ref,
                de_ref, dh_ref, tot_ref, dhs, wrow, misc_in, comb, comb_in, drb, drx, drt, dgacc, dgin, own, snd, d_in, x2, y2, x3, y3,
                d_ss, d_rs, x2_ss, x2_rs, y2_ss, y2_rs, x3_ss, x3_rs, y3_ss, y3_rs, o_sem, z_ss, z_rs, dh_sem, x_sem, m_ss, m_rs, c_ss, c_rs):
    i = pl.program_id(0)
    dp = lax.axis_index("dp")
    tp = lax.axis_index("tp")
    core = lax.rem(dp, 2)
    chip = dp // 2
    xi = lax.rem(chip, 2)
    yi = chip // 2
    chips = (chip, chip + 1 - 2 * xi, 3 - chip, chip + 2 - 4 * yi)
    sib = {"dp": dp + 1 - 2 * core}
    xn = {"dp": chips[1] * 2 + core}
    yn = {"dp": chips[3] * 2 + core}
    zn = {"tp": 1 - tp}
    half = SUB // 2
    zrows = dgacc.shape[0] // z_ss.shape[0]

    def remote(src, dst, ss, rs, to):
        return pltpu.make_async_remote_copy(src_ref=src, dst_ref=dst, send_sem=ss, recv_sem=rs, device_id=to, device_id_type=MESH)

    def d_copy(k):
        s = lax.rem(k, 2)
        return remote(snd, d_in.at[s], d_ss, d_rs.at[s], sib)

    def x2_copy(k):
        s, r = lax.rem(k, NSLOT), lax.rem(k, x2.shape[0])
        return remote(own.at[s, pl.ds(1, 2), pl.ds(0, half)], x2.at[r], x2_ss.at[s], x2_rs.at[r], xn)

    def y2_copy(k):
        s, r = lax.rem(k, NSLOT), lax.rem(k, y2.shape[0])
        return remote(own.at[s, pl.ds(2, 2), pl.ds(half, half)], y2.at[r], y2_ss.at[s], y2_rs.at[r], yn)

    def y3_copy(k):
        s = lax.rem(k, NSLOT)
        return remote(own.at[s, 3, pl.ds(0, half)], y3.at[s], y3_ss.at[s], y3_rs.at[s], yn)

    def x3_copy(k):
        s = lax.rem(k, NSLOT)
        return remote(own.at[s, 1, pl.ds(half, half)], x3.at[s], x3_ss.at[s], x3_rs.at[s], xn)

    def out_copy(k):
        s = lax.rem(k, NSLOT)
        return pltpu.make_async_copy(own.at[s, 0], de_ref.at[pl.ds(pl.multiple_of(k * SUB, SUB), SUB)], o_sem.at[s])

    def z_copy(q):
        rows = pl.ds(q * zrows, zrows)
        return remote(dgacc.at[rows], dgin.at[rows], z_ss.at[q], z_rs.at[q], zn)

    n_dp = misc_in.shape[0]

    def to_all(src, dst, ss, rs, j, arriving):
        slot = lax.rem(dp + (n_dp - j if arriving else 0), n_dp)
        return remote(src, dst.at[slot], ss.at[j], rs.at[j], {"dp": lax.rem(dp + j, n_dp)})

    @pl.when(i == 0)
    def _():
        barrier = pltpu.get_barrier_semaphore()
        for j in range(1, n_dp):
            pl.semaphore_signal(barrier, inc=1, device_id={"dp": lax.rem(dp + j, n_dp)}, device_id_type=MESH)
        pl.semaphore_signal(barrier, inc=1, device_id=zn, device_id_type=MESH)
        pl.semaphore_wait(barrier, n_dp)
        for j in range(1, n_dp):
            to_all(mine_ref, misc_in, m_ss, m_rs, j, False).start()
        dgacc[...] = jnp.zeros_like(dgacc)
        misc_in[dp] = mine_ref[...]
        for j in range(1, n_dp):
            to_all(mine_ref, misc_in, m_ss, m_rs, j, False).wait_send()
            to_all(mine_ref, misc_in, m_ss, m_rs, j, True).wait_recv()
        total = misc_in[0]
        for d in range(1, n_dp):
            total += misc_in[d]
        wrow[...] = row_ref[2] / total[0:1, :]
        tot_ref[16:24, :] = jnp.broadcast_to(total[1:2, :] / total[0:1, :], (8, LANES))

    def make_dr(er, tr, dr):
        raw = lax.dot_general(g_ref[...], er[...], NT, preferred_element_type=jnp.float32)
        for c in range(SUB // LANES):
            cols = slice(c * LANES, (c + 1) * LANES)
            th = jnp.tanh(raw[:, cols] * (1.0 / SOFT_CAP))
            ps = jnp.exp(SOFT_CAP * th - row_ref[0])
            pt = jnp.exp(tr[:, cols].astype(jnp.float32) - row_ref[1])
            dr[:, cols] = ((ps - pt) * wrow[...] * (1.0 - th * th)).astype(jnp.bfloat16)

    def add_dg(er, dr):
        for c in range(dgacc.shape[1] // 512):
            cols = slice(c * 512, (c + 1) * 512)
            dgacc[:, cols] += jnp.dot(dr[...], er[:, cols], preferred_element_type=jnp.float32)

    def second_stage():
        k = i - 1
        s = lax.rem(k, NSLOT)
        d_copy(k).wait()
        own[s] += d_in[lax.rem(k, 2)]
        x2_copy(k).start()
        y2_copy(k).start()

    @pl.when(i == 1)
    def _():
        second_stage()

    @pl.when((i >= 3) & (i < blocks + 3))
    def _():
        k = i - 3
        s, r = lax.rem(k, NSLOT), lax.rem(k, x2.shape[0])
        x2_copy(k).wait_recv()
        own[s, 0, 0:half] += x2[r, 0]
        own[s, 3, 0:half] += x2[r, 1]
        y3_copy(k).start()
        y2_copy(k).wait_recv()
        own[s, 1, half:] += y2[r, 0]
        x3_copy(k).start()
        own[s, 0, half:] += y2[r, 1]

    @pl.when(i < blocks)
    def _():
        make_dr(e_ref, t_ref, drb)
        drt[...] = drb[...].T

    @pl.when(i == base)
    def _():
        for q in range(z_ss.shape[0]):
            z_copy(q).start()
        pltpu.make_async_copy(x_ref, dhs, x_sem).start()

    @pl.when((i >= 2) & (i < blocks + 1))
    def _():
        second_stage()

    @pl.when(i < blocks)
    def _():
        s = lax.rem(i, NSLOT)
        for j in range(4):
            cols = pl.ds(pl.multiple_of((2 * chips[j] + 1 - core) * SUB, SUB), SUB)
            snd[j] = jnp.dot(drt[...], g_ref[:, cols], preferred_element_type=jnp.float32)
        d_copy(i).start()
        for j in range(4):
            cols = pl.ds(pl.multiple_of((2 * chips[j] + core) * SUB, SUB), SUB)
            own[s, j] = jnp.dot(drt[...], g_ref[:, cols], preferred_element_type=jnp.float32)

    @pl.when(i < base)
    def _():
        add_dg(e_ref, drb)

    @pl.when((i < base) & (lax.rem(i, 2) == 0))
    def _():
        make_dr(ex_ref, tx_ref, drx)

    @pl.when((i < base) & (lax.rem(i, 2) == 1))
    def _():
        add_dg(ex_ref, drx)

    @pl.when((i >= 5) & (i < blocks + 5))
    def _():
        k = i - 5
        s = lax.rem(k, NSLOT)
        y3_copy(k).wait_recv()
        own[s, 0, 0:half] += y3[s]
        x3_copy(k).wait_recv()
        own[s, 0, half:] += x3[s]
        out_copy(k).start()

    @pl.when(i >= 6)
    def _():
        k = i - 6
        x2_copy(k).wait_send()
        y2_copy(k).wait_send()
        x3_copy(k).wait_send()
        y3_copy(k).wait_send()
        out_copy(k).wait()

    @pl.when(i == blocks - 5)
    def _():
        for q in range(z_ss.shape[0]):
            z_copy(q).wait()
        pltpu.make_async_copy(x_ref, dhs, x_sem).wait()
        gain = 1.0 + w_ref[...]
        part = 128
        comb[...] = jnp.zeros_like(comb)

        @pl.loop(0, dgacc.shape[0] // part)
        def _(q):
            rows = pl.ds(pl.multiple_of(q * part, part), part)
            x = dhs[rows, :].astype(jnp.float32)
            dg = dgacc[rows, :] + dgin[rows, :]
            inv = lax.rsqrt(jnp.mean(x * x, axis=-1, keepdims=True) + NORM_EPS)
            dy = dg * gain
            dot = jnp.sum(dy * x, axis=-1, keepdims=True)
            dhs[rows, :] = (dy * inv - x * (dot * (inv * inv * inv) * (1.0 / x.shape[1]))).astype(jnp.bfloat16)
            dw = jnp.sum(dg * x * inv, axis=0, keepdims=True)
            for c in range(comb.shape[0]):
                comb[c:c + 1, :] += dw[:, c * LANES:(c + 1) * LANES]

        pltpu.make_async_copy(dhs, dh_ref, dh_sem).start()

    @pl.when(i == blocks - 4)
    def _():
        for j in range(1, n_dp):
            to_all(comb, comb_in, c_ss, c_rs, j, False).start()
        comb_in[dp] = comb[...]

    @pl.when(i == blocks + 5)
    def _():
        pltpu.make_async_copy(dhs, dh_ref, dh_sem).wait()
        for j in range(1, n_dp):
            to_all(comb, comb_in, c_ss, c_rs, j, False).wait_send()
            to_all(comb, comb_in, c_ss, c_rs, j, True).wait_recv()
        total = comb_in[0]
        for d in range(1, n_dp):
            total += comb_in[d]
        tot_ref[0:16, :] = total


def backward(g, hid, scale, row, mine, emb, teach, n_dp):
    rows, width = g.shape
    vocab = emb.shape[0]
    blocks = vocab // SUB
    base = blocks * 2 // 3
    last = blocks - 1

    def main(i):
        return jnp.minimum(i, last)

    def extra(i):
        return base + jnp.minimum(i // 2, blocks - base - 1)

    f32 = jnp.float32
    half = SUB // 2
    dma = pltpu.SemaphoreType.DMA
    return pl.pallas_call(
        functools.partial(grad_kernel, blocks, base),
        grid=(blocks + 6,),
        out_shape=(
            jax.ShapeDtypeStruct((vocab, SUB), f32),
            jax.ShapeDtypeStruct((rows, width), jnp.bfloat16),
            jax.ShapeDtypeStruct((width // LANES + 8, LANES), f32),
        ),
        in_specs=[
            pl.BlockSpec((rows, width), lambda i: (0, 0), pipeline_mode=pl.Buffered(1)),
            pl.BlockSpec(memory_space=pl.ANY),
            pl.BlockSpec((1, width), lambda i: (0, 0), pipeline_mode=pl.Buffered(1)),
            pl.BlockSpec((3, rows, LANES), lambda i: (0, 0, 0), pipeline_mode=pl.Buffered(1)),
            pl.BlockSpec((8, LANES), lambda i: (0, 0), pipeline_mode=pl.Buffered(1)),
            pl.BlockSpec((SUB, width), lambda i: (main(i), 0)),
            pl.BlockSpec((rows, SUB), lambda i: (0, main(i))),
            pl.BlockSpec((SUB, width), lambda i: (extra(i), 0)),
            pl.BlockSpec((rows, SUB), lambda i: (0, extra(i))),
        ],
        out_specs=(
            pl.BlockSpec(memory_space=pl.ANY),
            pl.BlockSpec(memory_space=pl.ANY),
            pl.BlockSpec((width // LANES + 8, LANES), lambda i: (0, 0)),
        ),
        scratch_shapes=[
            pltpu.VMEM((rows, width), jnp.bfloat16),
            pltpu.VMEM((rows, LANES), f32),
            pltpu.VMEM((n_dp, 8, LANES), f32),
            pltpu.VMEM((width // LANES, LANES), f32),
            pltpu.VMEM((n_dp, width // LANES, LANES), f32),
            pltpu.VMEM((rows, SUB), jnp.bfloat16),
            pltpu.VMEM((rows, SUB), jnp.bfloat16),
            pltpu.VMEM((SUB, rows), jnp.bfloat16),
            pltpu.VMEM((rows, width), f32),
            pltpu.VMEM((rows, width), f32),
            pltpu.VMEM((NSLOT, 4, SUB, SUB), f32),
            pltpu.VMEM((4, SUB, SUB), f32),
            pltpu.VMEM((2, 4, SUB, SUB), f32),
            pltpu.VMEM((4, 2, half, SUB), f32),
            pltpu.VMEM((4, 2, half, SUB), f32),
            pltpu.VMEM((NSLOT, half, SUB), f32),
            pltpu.VMEM((NSLOT, half, SUB), f32),
            dma, dma((2,)), dma((NSLOT,)), dma((4,)), dma((NSLOT,)), dma((4,)),
            dma((NSLOT,)), dma((NSLOT,)), dma((NSLOT,)), dma((NSLOT,)), dma((NSLOT,)), dma((4,)), dma((4,)), dma, dma,
            dma((n_dp,)), dma((n_dp,)), dma((n_dp,)), dma((n_dp,)),
        ],
        compiler_params=pltpu.CompilerParams(
            dimension_semantics=("arbitrary",), collective_id=0, has_side_effects=True, vmem_limit_bytes=62 * 1024 * 1024
        ),
        cost_estimate=pl.CostEstimate(
            flops=6 * rows * width * vocab, bytes_accessed=2 * vocab * (width + rows), transcendentals=3 * rows * vocab
        ),
        name="bwd_scatter",
    )(g, hid, scale, row, mine, emb, teach, emb, teach)


def solution(mesh):

    def device_fn(hid_loc, norm_w, emb_loc, teach_loc, mask_loc):
        mask_f32 = mask_loc.astype(jnp.float32)
        scale = norm_w.astype(jnp.float32)
        normed = rms_norm(hid_loc.astype(jnp.float32), scale).astype(jnp.bfloat16)
        part = forward_stats(normed, emb_loc, teach_loc)[:, :, 0]
        parts = lax.all_gather(part, "tp")
        top = jnp.max(parts[:, 0], axis=0)
        keep = jnp.exp(parts[:, 0] - top)
        tea_sum = jnp.sum(parts[:, 1] * keep, axis=0)
        cross = jnp.sum(parts[:, 2] * keep, axis=0)
        lse_tea = top + jnp.log(tea_sum)
        lse_stu = jnp.log(jnp.sum(parts[:, 3], axis=0))
        kl_tok = cross / tea_sum - lse_tea + lse_stu
        row = jnp.broadcast_to(jnp.stack([lse_stu, lse_tea, mask_f32])[:, :, None], (3, mask_f32.shape[0], LANES))
        sums = jnp.stack([jnp.sum(mask_f32), jnp.sum(mask_f32 * kl_tok)])
        mine = jnp.broadcast_to(jnp.pad(sums, (0, 6))[:, None], (8, LANES))
        grad_emb, grad_hid, total = backward(normed, hid_loc, scale[None, :], row, mine, emb_loc, teach_loc, mesh.shape["dp"])
        return total[-1, 0], grad_hid, grad_emb, total[:-8].reshape(-1)

    return jax.shard_map(device_fn, mesh=mesh, in_specs=(P('dp', None), P(None), P('tp', None), P('dp', 'tp'), P('dp')), out_specs=(P(), P('dp', None), P('tp', 'dp'), P(None)), check_vma=False)
```
